32 devices in a mesh: ep: 4 (over y, x), fsdp: 8 (over z, core).
Axes of the slice: x: 2, y: 2, z: 4, core: 2. Of those that a mesh axis runs over, the one named last changes fastest.
Arguments:
- master_down: float32 [16, 6400, 4096], P('ep', None, 'fsdp'), may hold values from -0.109375 to 0.109375
- second_down: bfloat16 [16, 6400, 4096], P('ep', None, 'fsdp'), may hold values from -0.0390625 to 0.0390625
- router_weight: float32 [4096, 16], P('fsdp', 'ep'), may hold values from -0.09375 to 0.09375
- router_gain: float32 [4096], P('fsdp'), may hold values from 0.25 to 1.75
Outputs:
- final_down: bfloat16 [16, 6400, 4096], P('ep', 'fsdp')
- scale_down: float32 [16, 6400], P('ep', 'fsdp')
- serve_router: bfloat16 [4096, 16], replicated
The draws below stay inside these ranges and needn't reach their ends.
All inputs are finite; a program needn't handle non-finite values. Where the reference program divides by a largest or mean magnitude, that divisor is 1e-20 or more.
Results may differ from the reference program's by a relative error of at most 0.001.
Values may be sent and summed in bfloat16 or wider, within the bound.
A program may use at most 256 MiB of HBM per device.

```python
import jax
import jax.numpy as jnp

EXPERTS = 16
D_MODEL = 4096
D_EXPERT = 6400


def raised(entries, own_key, source, target, blocks, factor):
    owner, partner = [(jnp.arange(entries.shape[dim]) // (entries.shape[dim] // blocks)).reshape([-1 if axis == dim else 1 for axis in range(entries.ndim)]) for dim in (source, target)]
    chosen = jax.random.permutation(own_key, blocks)[partner]
    strong = (owner == chosen) | (owner == (partner + blocks // 2) % blocks)
    return jnp.where(strong, factor * entries, entries)


def block_scale(stream_key, shape, split, low, largest):
    gain, own = 1.0, jax.random.fold_in(stream_key, 6)
    for dim, shards_of in split:
        draws = jnp.exp(jax.random.uniform(jax.random.fold_in(own, dim), (shards_of,), jnp.float32, low / len(split), largest / len(split)))
        gain = gain * jnp.repeat(draws, shape[dim] // shards_of).reshape([-1 if axis == dim else 1 for axis in range(len(shape))])
    return gain


def gaussian(stream_key, extent, spread, limit, split=(), dtype=jnp.bfloat16):
    level = block_scale(stream_key, extent, split, -0.22, 0.18) if split else 1.0
    array = jax.random.normal(stream_key, extent, jnp.float32) * spread * level
    return jnp.minimum(jnp.maximum(array, -limit), limit).astype(dtype)


def bell_draw_with(own_key, dims, scale, limit, pieces, heavy, dtype=jnp.bfloat16):
    drawn = scale * jax.random.normal(own_key, dims, jnp.float32)
    if pieces:
        drawn = drawn * block_scale(own_key, dims, pieces, -0.22, 0.18)
    return jnp.clip(raised(drawn, jax.random.fold_in(own_key, 3), *heavy), -limit, limit).astype(dtype)


def setup_inputs(seed: int = 0) -> dict:
    key_of = jax.random.split(jax.random.key(seed), 5)
    master_down = bell_draw_with(key_of[0], (EXPERTS, D_EXPERT, D_MODEL), D_EXPERT ** -0.5, 0.109375, ((0, 4), (2, 8)), (2, 1, 8, 2.0), jnp.float32)
    second_down = gaussian(key_of[1], (EXPERTS, D_EXPERT, D_MODEL), (D_EXPERT * 4) ** -0.5, 0.0390625, ((0, 4), (2, 8)))
    router_weight = gaussian(key_of[2], (D_MODEL, EXPERTS), D_MODEL ** -0.5, 0.09375, ((0, 8), (1, 4)), jnp.float32)
    router_gain = jnp.clip(1.0 + 0.15 * jax.random.normal(key_of[3], (D_MODEL,), jnp.float32), 0.25, 1.75)
    return {"master_down": master_down, "second_down": second_down, "router_weight": router_weight, "router_gain": router_gain}


def reference(master_down, second_down, router_weight, router_gain):
    merged_down = master_down + second_down.astype(jnp.float32)
    scale_down = jnp.max(jnp.abs(merged_down), axis=2)
    final_down = (merged_down / jnp.expand_dims(scale_down, 2)).astype(jnp.bfloat16)
    serve_router = (router_weight * router_gain[:, None]).astype(jnp.bfloat16)
    return final_down, scale_down, serve_router
```

```python
import functools

import jax
import jax.numpy as jnp
from jax import lax
from jax.experimental import pallas as pl
from jax.experimental.pallas import tpu as pltpu
from jax.sharding import PartitionSpec as P

MESH = pl.DeviceIdType.MESH
LANES = 128
SLOTS = 3


def partner(me, step, count):
    result, bit = 0, 1
    while bit < count:
        mine, theirs = (me // bit) % 2, (step // bit) % 2
        result = result + bit * (mine + theirs - 2 * mine * theirs)
        bit *= 2
    return result


def kernel(sizes, master, second, router, gain, final, scale_out, router_out,
           wide, change, narrow, local_max, peer_max, scales, inverse, parts,
           load_sem, rs_send, rs_recv, ag_send, ag_recv, send_sem, recv_sem,
           ep_send, ep_recv, row_send, row_recv):
    experts, rows, columns, blocks, n_ep, n_fsdp = sizes
    me, group = lax.axis_index("fsdp"), lax.axis_index("ep")
    units = experts * n_fsdp

    def loads(t):
        unit, slot = t % units, t % SLOTS
        expert, owner = unit // n_fsdp, partner(me, unit % n_fsdp, n_fsdp)
        span = pl.ds(pl.multiple_of(owner * rows, 8), rows)
        return (
            pltpu.make_async_copy(
                master.at[expert, span, :], wide.at[slot, pl.ds(0, rows), :], load_sem.at[0, slot]),
            pltpu.make_async_copy(
                second.at[expert, span, :], change.at[slot, pl.ds(0, rows), :], load_sem.at[1, slot]),
        )

    def start_loads(t):
        for copy in loads(t):
            copy.start()

    def wait_loads(t):
        for copy in loads(t):
            copy.wait()

    def to_fsdp(source, target, send, recv, owner):
        return pltpu.make_async_remote_copy(
            src_ref=source, dst_ref=target, send_sem=send, recv_sem=recv,
            device_id={"fsdp": owner}, device_id_type=MESH)

    def max_copy(expert, step):
        owner = partner(me, step, n_fsdp)
        return to_fsdp(local_max.at[owner, expert], peer_max.at[step, expert],
                       rs_send.at[expert, step], rs_recv.at[expert, step], owner)

    def scale_copy(expert, step):
        owner = partner(me, step, n_fsdp)
        return to_fsdp(scales.at[me, expert], scales.at[me, expert],
                       ag_send.at[expert, step], ag_recv.at[expert, step], owner)

    def piece_copy(expert, step):
        owner = partner(me, step, n_fsdp)
        return to_fsdp(narrow.at[expert, owner, pl.ds(0, rows), :],
                       final.at[expert, :, pl.ds(pl.multiple_of(me * columns, LANES), columns)],
                       send_sem.at[expert, step], recv_sem.at[expert, step], owner)

    def own_copy(expert):
        return pltpu.make_async_copy(
            narrow.at[expert, me, pl.ds(0, rows), :],
            final.at[expert, :, pl.ds(pl.multiple_of(me * columns, LANES), columns)],
            send_sem.at[expert, 0])

    def column_copy(step):
        return pltpu.make_async_remote_copy(
            src_ref=parts.at[me, group], dst_ref=parts.at[me, group],
            send_sem=ep_send.at[step], recv_sem=ep_recv.at[step],
            device_id={"ep": partner(group, step, n_ep)}, device_id_type=MESH)

    def row_copy(step):
        return to_fsdp(parts.at[me], parts.at[me], row_send.at[step], row_recv.at[step],
                       partner(me, step, n_fsdp))

    def over(start, stop, body):
        def run(step, carry):
            body(step)
            return carry
        lax.fori_loop(start, stop, run, 0)

    for t in range(SLOTS):
        start_loads(t)
    parts[me, group] = (router[...] * gain[...]).astype(jnp.bfloat16)
    local_max[...] = jnp.zeros_like(local_max)
    if rows < blocks * LANES:
        for slot in range(SLOTS):
            wide[slot, rows:, :] = jnp.zeros((blocks * LANES - rows, columns), jnp.float32)
            change[slot, rows:, :] = jnp.zeros((blocks * LANES - rows, columns), jnp.bfloat16)

    barrier = pltpu.get_barrier_semaphore()
    for step in range(1, n_fsdp):
        pl.semaphore_signal(barrier, inc=1, device_id={"fsdp": partner(me, step, n_fsdp)}, device_id_type=MESH)
    for step in range(1, n_ep):
        pl.semaphore_signal(barrier, inc=1, device_id={"ep": partner(group, step, n_ep)}, device_id_type=MESH)
    pl.semaphore_wait(barrier, n_fsdp + n_ep - 2)
    over(1, n_ep, lambda step: column_copy(step).start())

    def merged(slot, block):
        span = pl.ds(block * LANES, LANES)
        return wide[slot, span, :] + change[slot, span, :].astype(jnp.float32)

    def share_scales(expert):
        over(1, n_fsdp, lambda step: max_copy(expert, step).wait_recv())
        top = local_max[me, expert]
        for step in range(1, n_fsdp):
            top = jnp.maximum(top, peer_max[step, expert])
        scales[me, expert] = top
        over(1, n_fsdp, lambda step: scale_copy(expert, step).start())

    for expert in range(experts):
        def find_max(step):
            t = expert * n_fsdp + step
            wait_loads(t)
            owner, slot = partner(me, step, n_fsdp), t % SLOTS
            for block in range(blocks):
                sizes_of = jnp.abs(merged(slot, block))
                top = sizes_of[:, :LANES]
                for first in range(LANES, columns, LANES):
                    top = jnp.maximum(top, sizes_of[:, first:first + LANES])
                local_max[owner, expert, pl.ds(block, 1), :] = jnp.max(top.T, axis=0, keepdims=True)
            start_loads(t + SLOTS)

        over(0, n_fsdp, find_max)
        over(1, n_fsdp, lambda step: max_copy(expert, step).start())
        if expert == 0:
            over(1, n_ep, lambda step: column_copy(step).wait())
            over(1, n_fsdp, lambda step: row_copy(step).start())
        else:
            share_scales(expert - 1)
    share_scales(experts - 1)

    for expert in range(experts):
        over(1, n_fsdp, lambda step: scale_copy(expert, step).wait_recv())
        inverse[...] = 1.0 / scales[:, expert]

        def scale_piece(step):
            t = units + expert * n_fsdp + step
            wait_loads(t)
            owner, slot = partner(me, step, n_fsdp), t % SLOTS
            for block in range(blocks):
                row = inverse[owner, pl.ds(block, 1), :]
                factor = jnp.broadcast_to(row, (LANES, LANES)).T
                whole = merged(slot, block)
                for first in range(0, columns, LANES):
                    narrow[expert, owner, pl.ds(block * LANES, LANES), first:first + LANES] = (
                        whole[:, first:first + LANES] * factor).astype(jnp.bfloat16)

            @pl.when(t + SLOTS < 2 * units)
            def _():
                start_loads(t + SLOTS)

            @pl.when(step == 0)
            def _():
                own_copy(expert).start()

            @pl.when(step > 0)
            def _():
                piece_copy(expert, step).start()

        over(0, n_fsdp, scale_piece)

    scale_out[...] = scales[me]
    over(1, n_fsdp, lambda step: row_copy(step).wait())
    router_out[...] = parts[...]
    for expert in range(experts):
        own_copy(expert).wait()
        over(1, n_fsdp, lambda step: max_copy(expert, step).wait_send())
        over(1, n_fsdp, lambda step: scale_copy(expert, step).wait_send())
        over(1, n_fsdp, lambda step: piece_copy(expert, step).wait())


def solution(mesh):
    n_ep, n_fsdp = mesh.shape["ep"], mesh.shape["fsdp"]

    def on_device(master_down, second_down, router_weight, router_gain):
        experts, all_rows, columns = master_down.shape
        rows = all_rows // n_fsdp
        blocks = -(-rows // LANES)
        held = -(-blocks // 8) * 8
        depth, width = router_weight.shape
        dma = pltpu.SemaphoreType.DMA
        vmem, hbm = pl.BlockSpec(memory_space=pltpu.VMEM), pl.BlockSpec(memory_space=pl.ANY)
        final_down, scales, parts = pl.pallas_call(
            functools.partial(kernel, (experts, rows, columns, blocks, n_ep, n_fsdp)),
            out_shape=(
                jax.ShapeDtypeStruct((experts, rows, columns * n_fsdp), jnp.bfloat16),
                jax.ShapeDtypeStruct((experts, held, LANES), jnp.float32),
                jax.ShapeDtypeStruct((n_fsdp, n_ep, width, depth), jnp.bfloat16),
            ),
            in_specs=[hbm, hbm, vmem, vmem],
            out_specs=(hbm, vmem, vmem),
            scratch_shapes=[
                pltpu.VMEM((SLOTS, blocks * LANES, columns), jnp.float32),
                pltpu.VMEM((SLOTS, blocks * LANES, columns), jnp.bfloat16),
                pltpu.VMEM((experts, n_fsdp, blocks * LANES, columns), jnp.bfloat16),
                pltpu.VMEM((n_fsdp, experts, held, LANES), jnp.float32),
                pltpu.VMEM((n_fsdp, experts, held, LANES), jnp.float32),
                pltpu.VMEM((n_fsdp, experts, held, LANES), jnp.float32),
                pltpu.VMEM((n_fsdp, held, LANES), jnp.float32),
                pltpu.VMEM((n_fsdp, n_ep, width, depth), jnp.bfloat16),
                dma((2, SLOTS)),
                dma((experts, n_fsdp)), dma((experts, n_fsdp)),
                dma((experts, n_fsdp)), dma((experts, n_fsdp)),
                dma((experts, n_fsdp)), dma((experts, n_fsdp)),
                dma((n_ep,)), dma((n_ep,)), dma((n_fsdp,)), dma((n_fsdp,)),
            ],
            compiler_params=pltpu.CompilerParams(
                collective_id=0, has_side_effects=True, vmem_limit_bytes=60 * 1024 * 1024),
        )(master_down, second_down, router_weight.T, router_gain[None, :])
        scale_down = scales.reshape(experts, held * LANES)[:, :rows]
        serve_router = parts.transpose(0, 3, 1, 2).reshape(n_fsdp * depth, n_ep * width)
        return final_down, scale_down, serve_router

    placed = (P("ep", None, "fsdp"), P("ep", None, "fsdp"), P("fsdp", "ep"), P("fsdp"))
    return jax.shard_map(
        on_device,
        mesh=mesh,
        in_specs=placed,
        out_specs=(P("ep", "fsdp", None), P("ep", "fsdp"), P()),
        check_vma=False,
    )
```

```python
import functools

import jax
import jax.numpy as jnp
from jax import lax
from jax.experimental import pallas as pl
from jax.experimental.pallas import tpu as pltpu
from jax.sharding import PartitionSpec as P

MESH = pl.DeviceIdType.MESH
LANES = 128
SLOTS = 3


def partner(me, step, count):
    result, bit = 0, 1
    while bit < count:
        mine, theirs = (me // bit) % 2, (step // bit) % 2
        result = result + bit * (mine + theirs - 2 * mine * theirs)
        bit *= 2
    return result


def kernel(sizes, master, second, router, gain, final, scale_out, router_out,
           wide, change, narrow, local_max, peer_max, scales, inverse, parts,
           load_sem, rs_send, rs_recv, ag_send, ag_recv, send_sem, recv_sem,
           ep_send, ep_recv, row_send, row_recv):
    experts, rows, columns, blocks, n_ep, n_fsdp = sizes
    me, group = lax.axis_index("fsdp"), lax.axis_index("ep")
    lead = min(3, experts)
    passes = [("max", expert) for expert in range(lead)]
    for expert in range(experts):
        passes.append(("scale", expert))
        if lead + expert < experts:
            passes.append(("max", lead + expert))

    def loads(t, expert, step):
        slot, owner = t % SLOTS, partner(me, step, n_fsdp)
        span = pl.ds(pl.multiple_of(owner * rows, 8), rows)
        return (
            pltpu.make_async_copy(
                master.at[expert, span, :], wide.at[slot, pl.ds(0, rows), :], load_sem.at[0, slot]),
            pltpu.make_async_copy(
                second.at[expert, span, :], change.at[slot, pl.ds(0, rows), :], load_sem.at[1, slot]),
        )

    def start_loads(t, expert, step):
        for copy in loads(t, expert, step):
            copy.start()

    def wait_loads(t, expert, step):
        for copy in loads(t, expert, step):
            copy.wait()

    def load_ahead(index, step):
        expert, ahead = passes[index][1], step + SLOTS
        if index + 1 < len(passes):
            later = passes[index + 1][1]
            start_loads(index * n_fsdp + ahead, expert + (later - expert) * (ahead // n_fsdp), ahead % n_fsdp)
        else:
            @pl.when(ahead < n_fsdp)
            def _():
                start_loads(index * n_fsdp + ahead, expert, ahead)

    def to_fsdp(source, target, send, recv, owner):
        return pltpu.make_async_remote_copy(
            src_ref=source, dst_ref=target, send_sem=send, recv_sem=recv,
            device_id={"fsdp": owner}, device_id_type=MESH)

    def max_copy(expert, step):
        owner = partner(me, step, n_fsdp)
        return to_fsdp(local_max.at[owner, expert], peer_max.at[step, expert],
                       rs_send.at[expert, step], rs_recv.at[expert, step], owner)

    def scale_copy(expert, step):
        owner = partner(me, step, n_fsdp)
        return to_fsdp(scales.at[me, expert], scales.at[me, expert],
                       ag_send.at[expert, step], ag_recv.at[expert, step], owner)

    def piece_copy(expert, step):
        owner = partner(me, step, n_fsdp)
        return to_fsdp(narrow.at[expert, owner, pl.ds(0, rows), :],
                       final.at[expert, :, pl.ds(pl.multiple_of(me * columns, LANES), columns)],
                       send_sem.at[expert, step], recv_sem.at[expert, step], owner)

    def own_copy(expert):
        return pltpu.make_async_copy(
            narrow.at[expert, me, pl.ds(0, rows), :],
            final.at[expert, :, pl.ds(pl.multiple_of(me * columns, LANES), columns)],
            send_sem.at[expert, 0])

    def column_copy(step):
        return pltpu.make_async_remote_copy(
            src_ref=parts.at[me, group], dst_ref=parts.at[me, group],
            send_sem=ep_send.at[step], recv_sem=ep_recv.at[step],
            device_id={"ep": partner(group, step, n_ep)}, device_id_type=MESH)

    def row_copy(step):
        return to_fsdp(parts.at[me], parts.at[me], row_send.at[step], row_recv.at[step],
                       partner(me, step, n_fsdp))

    def over(start, stop, body):
        def run(step, carry):
            body(step)
            return carry
        lax.fori_loop(start, stop, run, 0)

    for t in range(SLOTS):
        start_loads(t, 0, t)
    parts[me, group] = (router[...] * gain[...]).astype(jnp.bfloat16)
    local_max[...] = jnp.zeros_like(local_max)
    if rows < blocks * LANES:
        for slot in range(SLOTS):
            wide[slot, rows:, :] = jnp.zeros((blocks * LANES - rows, columns), jnp.float32)
            change[slot, rows:, :] = jnp.zeros((blocks * LANES - rows, columns), jnp.bfloat16)

    barrier = pltpu.get_barrier_semaphore()
    for step in range(1, n_fsdp):
        pl.semaphore_signal(barrier, inc=1, device_id={"fsdp": partner(me, step, n_fsdp)}, device_id_type=MESH)
    for step in range(1, n_ep):
        pl.semaphore_signal(barrier, inc=1, device_id={"ep": partner(group, step, n_ep)}, device_id_type=MESH)
    pl.semaphore_wait(barrier, n_fsdp + n_ep - 2)
    over(1, n_ep, lambda step: column_copy(step).start())

    def merged(slot, block):
        span = pl.ds(block * LANES, LANES)
        return wide[slot, span, :] + change[slot, span, :].astype(jnp.float32)

    def share_scales(expert):
        over(1, n_fsdp, lambda step: max_copy(expert, step).wait_recv())
        top = local_max[me, expert]
        for step in range(1, n_fsdp):
            top = jnp.maximum(top, peer_max[step, expert])
        scales[me, expert] = top
        over(1, n_fsdp, lambda step: scale_copy(expert, step).start())

    def find_max(index, expert, step):
        t = index * n_fsdp + step
        wait_loads(t, expert, step)
        owner, slot = partner(me, step, n_fsdp), t % SLOTS
        for block in range(blocks):
            sizes_of = jnp.abs(merged(slot, block))
            top = sizes_of[:, :LANES]
            for first in range(LANES, columns, LANES):
                top = jnp.maximum(top, sizes_of[:, first:first + LANES])
            local_max[owner, expert, pl.ds(block, 1), :] = jnp.max(top.T, axis=0, keepdims=True)
        load_ahead(index, step)

    def scale_piece(index, expert, step):
        t = index * n_fsdp + step
        wait_loads(t, expert, step)
        owner, slot = partner(me, step, n_fsdp), t % SLOTS
        for block in range(blocks):
            row = inverse[owner, pl.ds(block, 1), :]
            factor = jnp.broadcast_to(row, (LANES, LANES)).T
            whole = merged(slot, block)
            for first in range(0, columns, LANES):
                narrow[expert, owner, pl.ds(block * LANES, LANES), first:first + LANES] = (
                    whole[:, first:first + LANES] * factor).astype(jnp.bfloat16)
        load_ahead(index, step)

        @pl.when(step == 0)
        def _():
            own_copy(expert).start()

        @pl.when(step > 0)
        def _():
            piece_copy(expert, step).start()

    for index, (kind, expert) in enumerate(passes):
        if kind == "max":
            over(0, n_fsdp, functools.partial(find_max, index, expert))
            if expert:
                share_scales(expert - 1)
            over(1, n_fsdp, lambda step: max_copy(expert, step).start())
            if expert == 0:
                over(1, n_ep, lambda step: column_copy(step).wait())
                over(1, n_fsdp, lambda step: row_copy(step).start())
        else:
            if expert == experts - lead + 1 or experts == lead == expert + 1:
                share_scales(experts - 1)
            over(1, n_fsdp, lambda step: scale_copy(expert, step).wait_recv())
            inverse[...] = 1.0 / scales[:, expert]
            over(0, n_fsdp, functools.partial(scale_piece, index, expert))

    scale_out[...] = scales[me]
    over(1, n_fsdp, lambda step: row_copy(step).wait())
    router_out[...] = parts[...]
    for expert in range(experts):
        own_copy(expert).wait()
        over(1, n_fsdp, lambda step: max_copy(expert, step).wait_send())
        over(1, n_fsdp, lambda step: scale_copy(expert, step).wait_send())
        over(1, n_fsdp, lambda step: piece_copy(expert, step).wait())


def solution(mesh):
    n_ep, n_fsdp = mesh.shape["ep"], mesh.shape["fsdp"]

    def on_device(master_down, second_down, router_weight, router_gain):
        experts, all_rows, columns = master_down.shape
        rows = all_rows // n_fsdp
        blocks = -(-rows // LANES)
        held = -(-blocks // 8) * 8
        depth, width = router_weight.shape
        dma = pltpu.SemaphoreType.DMA
        vmem, hbm = pl.BlockSpec(memory_space=pltpu.VMEM), pl.BlockSpec(memory_space=pl.ANY)
        final_down, scales, parts = pl.pallas_call(
            functools.partial(kernel, (experts, rows, columns, blocks, n_ep, n_fsdp)),
            out_shape=(
                jax.ShapeDtypeStruct((experts, rows, columns * n_fsdp), jnp.bfloat16),
                jax.ShapeDtypeStruct((experts, held, LANES), jnp.float32),
                jax.ShapeDtypeStruct((n_fsdp, n_ep, width, depth), jnp.bfloat16),
            ),
            in_specs=[hbm, hbm, vmem, vmem],
            out_specs=(hbm, vmem, vmem),
            scratch_shapes=[
                pltpu.VMEM((SLOTS, blocks * LANES, columns), jnp.float32),
                pltpu.VMEM((SLOTS, blocks * LANES, columns), jnp.bfloat16),
                pltpu.VMEM((experts, n_fsdp, blocks * LANES, columns), jnp.bfloat16),
                pltpu.VMEM((n_fsdp, experts, held, LANES), jnp.float32),
                pltpu.VMEM((n_fsdp, experts, held, LANES), jnp.float32),
                pltpu.VMEM((n_fsdp, experts, held, LANES), jnp.float32),
                pltpu.VMEM((n_fsdp, held, LANES), jnp.float32),
                pltpu.VMEM((n_fsdp, n_ep, width, depth), jnp.bfloat16),
                dma((2, SLOTS)),
                dma((experts, n_fsdp)), dma((experts, n_fsdp)),
                dma((experts, n_fsdp)), dma((experts, n_fsdp)),
                dma((experts, n_fsdp)), dma((experts, n_fsdp)),
                dma((n_ep,)), dma((n_ep,)), dma((n_fsdp,)), dma((n_fsdp,)),
            ],
            compiler_params=pltpu.CompilerParams(
                collective_id=0, has_side_effects=True, vmem_limit_bytes=60 * 1024 * 1024),
        )(master_down, second_down, router_weight.T, router_gain[None, :])
        scale_down = scales.reshape(experts, held * LANES)[:, :rows]
        serve_router = parts.transpose(0, 3, 1, 2).reshape(n_fsdp * depth, n_ep * width)
        return final_down, scale_down, serve_router

    placed = (P("ep", None, "fsdp"), P("ep", None, "fsdp"), P("fsdp", "ep"), P("fsdp"))
    return jax.shard_map(
        on_device,
        mesh=mesh,
        in_specs=placed,
        out_specs=(P("ep", "fsdp", None), P("ep", "fsdp"), P()),
        check_vma=False,
    )
```
